32 devices in a mesh: replica: 1 (over z), data2: 4 (over y), data: 8 (over x, core).
Axes of the slice: x: 4, y: 4, z: 1, core: 2. Of those that a mesh axis runs over, the one named last changes fastest.
The devices are a block of a 4x4x8 slice.
Arguments:
- q_hidden: bfloat16 [32, 32, 1024], P(('replica', 'data2', 'data'))
- d_hidden: bfloat16 [32, 8192, 1024], P(('replica', 'data2', 'data'))
- w_proj: bfloat16 [1024, 128], replicated
- q_mask: int32 [32, 32], P(('replica', 'data2', 'data'))
- d_mask: int32 [32, 8192], P(('replica', 'data2', 'data'))
- temperature: float32 [], replicated
Outputs:
- output 1: float32 [32], P(('replica', 'data2', 'data'))
- output 2: float32 [1], P('replica')
All inputs are finite; a program needn't handle non-finite values.
Results may differ from the reference program's by a relative error of at most 0.00151.
Values are sent between devices in bfloat16 or wider.
A program may use at most 768 MiB of HBM per device.

```python
import math
import jax
import jax.numpy as jnp
from jax import lax

BATCH = 32
QLEN = 32
DLEN = 8192
HIDDEN = 1024
PROJ = 128

NORM_EPS = 1e-6
TAU_SCALE = QLEN / (8.0 * math.log(BATCH))


def setup_inputs(seed: int = 0, part: int = 0) -> dict:
    base_key = jax.random.key(seed)
    rand_keys = jax.random.split(jax.random.fold_in(base_key, part), 7)
    shared = jax.random.normal(rand_keys[0], (HIDDEN,), jnp.float32)
    doc_len = jax.random.randint(rand_keys[1], (BATCH,), DLEN // 2, DLEN + 1)
    qry_len = jax.random.randint(rand_keys[2], (BATCH,), QLEN // 2, QLEN + 1)
    doc_mask = (jnp.arange(DLEN)[None, :] < doc_len[:, None]).astype(jnp.int32)
    qry_mask = (jnp.arange(QLEN)[None, :] < qry_len[:, None]).astype(jnp.int32)
    doc_noise = jax.random.normal(rand_keys[3], (BATCH, DLEN, HIDDEN), jnp.float32)
    src_pos = jax.random.randint(rand_keys[4], (BATCH, QLEN), 0, doc_len[:, None])
    src_idx = jnp.broadcast_to(src_pos[:, :, None], (BATCH, QLEN, HIDDEN))
    copied = jnp.take_along_axis(doc_noise, src_idx, axis=1)
    share_w = jax.random.uniform(rand_keys[5], (BATCH, 1, 1), jnp.float32, 0.15, 0.4)
    fresh = jax.random.normal(rand_keys[6], (BATCH, QLEN, HIDDEN), jnp.float32)
    half_amp = math.sqrt(0.5)
    d_keep = doc_mask[:, :, None] > 0
    d_hidden = jnp.where(d_keep, half_amp, 2.0) * shared + jnp.where(d_keep, half_amp, 0.3) * doc_noise
    q_keep = qry_mask[:, :, None] > 0
    q_mix = jnp.sqrt(share_w) * copied + jnp.sqrt(1.0 - share_w) * fresh
    q_body = jnp.where(q_keep, q_mix, copied)
    q_hidden = jnp.where(q_keep, 1.0, 2.5) * (half_amp * shared + half_amp * q_body)
    w_proj = jax.random.normal(jax.random.fold_in(base_key, 1000), (HIDDEN, PROJ), jnp.float32) * HIDDEN ** -0.5
    temperature = jax.random.uniform(jax.random.fold_in(base_key, 2000), (), jnp.float32, 0.6, 1.4) * TAU_SCALE
    return {
        'q_hidden': q_hidden.astype(jnp.bfloat16),
        'd_hidden': d_hidden.astype(jnp.bfloat16),
        'w_proj': w_proj.astype(jnp.bfloat16),
        'q_mask': qry_mask,
        'd_mask': doc_mask,
        'temperature': temperature.astype(jnp.float32),
    }


def project(hidden, w_proj):
    flat_rows = hidden.reshape(-1, hidden.shape[-1])
    proj_f32 = jnp.dot(flat_rows, w_proj, preferred_element_type=jnp.float32)
    row_norm = jnp.sqrt(jnp.sum(proj_f32 * proj_f32, axis=-1, keepdims=True) + NORM_EPS)
    unit_rows = (proj_f32 / row_norm).astype(jnp.bfloat16)
    return unit_rows.reshape(hidden.shape[:-1] + (w_proj.shape[1],))


def reference(q_hidden, d_hidden, w_proj, q_mask, d_mask, temperature):
    q_tok = project(q_hidden, w_proj).astype(jnp.float32)
    d_tok = project(d_hidden, w_proj).astype(jnp.float32)
    d_valid = d_mask > 0
    q_weight = q_mask.astype(jnp.float32)

    def score_row(row_in):
        q_row, weight_row = row_in
        sim_vals = jnp.einsum('td,psd->tps', q_row, d_tok)
        best_sim = jnp.max(jnp.where(d_valid[None], sim_vals, -jnp.inf), axis=-1)
        return jnp.sum(weight_row[:, None] * best_sim, axis=0)

    scores = lax.map(score_row, (q_tok, q_weight))
    logits = scores / temperature
    row_max = jnp.max(logits, axis=1, keepdims=True)
    log_norm = row_max[:, 0] + jnp.log(jnp.sum(jnp.exp(logits - row_max), axis=1))
    loss_rows = log_norm - jnp.diagonal(logits)
    return loss_rows, jnp.mean(loss_rows).reshape(1)
```

```python
import functools

import jax
import jax.numpy as jnp
from jax import lax
from jax.experimental import pallas as pl
from jax.experimental.pallas import tpu as pltpu
from jax.sharding import PartitionSpec as P

NORM_EPS = 1e-6
ROW_AXES = ('replica', 'data2', 'data')
MASKED = -1e30
CORES = 2
CHUNK = 512
DEPTH = 6
UNROLL = 2
SEND_STEP = 3
SCORE_ROWS = 4096
GROUP = 8
MESH = pl.DeviceIdType.MESH


def ring_distance(step, size):
    return min(step, size - step)


def peer_offsets(outer, inner):
    chips = inner // CORES
    offsets = [(a, b, c) for a in range(outer) for b in range(chips) for c in range(CORES)]
    return sorted(offsets, key=lambda o: (ring_distance(o[0], outer) + ring_distance(o[1], chips), o[2], o[0], o[1]))


def kernel(outer, inner, q_hbm, d_ref, w_hbm, qm_hbm, dm_hbm, out_ref,
           hidden, raw, tokens, all_q, acc, column, table, senders, q_ref, w_ref, qm_ref, dm_ref,
           small_sem, chunk_sem, send_sem, q_sem, s_send_sem, s_sem):
    group_size = outer * inner
    chips = inner // CORES
    q_len, proj = all_q.shape[1], w_ref.shape[1]
    n_chunks = hidden.shape[0]
    offsets = peer_offsets(outer, inner)
    my_outer, my_inner = lax.axis_index('data2'), lax.axis_index('data')
    my_chip, my_core = my_inner // CORES, my_inner % CORES
    me = my_outer * inner + my_inner

    def device(offset, sign):
        a, b, c = offset
        a = lax.rem(my_outer + sign * a + outer, outer)
        b = lax.rem(my_chip + sign * b + chips, chips)
        c = lax.rem(my_core + sign * c + CORES, CORES)
        return a, b * CORES + c

    def device_id(offset):
        a, b = device(offset, 1)
        return {'data2': a, 'data': b}

    def row_of(p):
        per_row = 128 // q_len
        row = p % per_row * (group_size // per_row) + p // per_row
        return slice(row, row + 1)

    smalls = [pltpu.make_async_copy(src, dst, small_sem.at[i]) for i, (src, dst) in enumerate(
        [(q_hbm, q_ref), (w_hbm, w_ref), (qm_hbm, qm_ref), (dm_hbm, dm_ref)])]
    for copy in smalls:
        copy.start()

    def fetch(b):
        return pltpu.make_async_copy(d_ref.at[0, pl.ds(b * CHUNK, CHUNK), :], hidden.at[b], chunk_sem.at[b])

    barrier = pltpu.get_barrier_semaphore()
    for offset in offsets[1:]:
        pl.semaphore_signal(barrier, inc=1, device_id=device_id(offset), device_id_type=MESH)

    for b in range(DEPTH):
        fetch(b).start()

    for p in range(group_size):
        a, b = device(offsets[p], -1)
        senders[row_of(p), :] = jnp.full((1, 128), a * inner + b, jnp.int32)
    for copy in smalls:
        copy.wait()

    y = jnp.dot(q_ref[0], w_ref[...], preferred_element_type=jnp.float32)
    unit = y * lax.rsqrt(jnp.sum(y * y, axis=-1, keepdims=True) + NORM_EPS)
    row = lax.broadcasted_iota(jnp.int32, (q_len, q_len), 0)
    col = lax.broadcasted_iota(jnp.int32, (q_len, q_len), 1)
    weight = jnp.sum(jnp.where(row == col, qm_ref[...], 0).astype(jnp.float32), axis=1, keepdims=True)
    all_q[0] = jnp.where(weight > 0, unit, 0.0).astype(jnp.bfloat16)

    def q_copy(p):
        return pltpu.make_async_remote_copy(
            src_ref=all_q.at[0], dst_ref=all_q.at[p], send_sem=send_sem, recv_sem=q_sem.at[p // GROUP],
            device_id=device_id(offsets[p]), device_id_type=MESH)

    def project(b, slot):
        raw[slot] = jnp.dot(hidden[b], w_ref[...], preferred_element_type=jnp.float32)

    def normalise(b, slot):
        y = raw[slot]
        scale = lax.rsqrt(jnp.sum(y * y, axis=-1, keepdims=True) + NORM_EPS)
        rows = pl.ds(pl.multiple_of(b * CHUNK, CHUNK), CHUNK)
        tokens[rows, :proj] = (y * scale).astype(jnp.bfloat16)
        mask = dm_ref[:, rows]
        bias = jnp.where(mask > 0, 0.0, MASKED)
        for c in range(0, CHUNK, 128):
            block = jnp.broadcast_to(bias[:, c:c + 128], (128, 128)).T
            tokens[pl.ds(pl.multiple_of(b * CHUNK + c, 128), 128), proj:] = block.astype(jnp.bfloat16)

    def step(i, first):
        for u in range(UNROLL):
            fetch(i * UNROLL + u).wait()
        for u in range(UNROLL):
            @pl.when(i * UNROLL + u + DEPTH < n_chunks)
            def _():
                fetch(i * UNROLL + u + DEPTH).start()
        if not first:
            for u in range(UNROLL):
                normalise((i - 1) * UNROLL + u, lax.rem(i + 1, 2) * UNROLL + u)
        for u in range(UNROLL):
            project(i * UNROLL + u, lax.rem(i, 2) * UNROLL + u)

    steps = n_chunks // UNROLL
    step(0, True)

    @pl.loop(1, SEND_STEP)
    def _(i):
        step(i, False)

    pl.semaphore_wait(barrier, group_size - 1)
    for p in range(1, group_size):
        q_copy(p).start()

    @pl.loop(SEND_STEP, steps)
    def _(i):
        step(i, False)

    for u in range(UNROLL):
        normalise((steps - 1) * UNROLL + u, (steps - 1) % 2 * UNROLL + u)

    lane = lax.broadcasted_iota(jnp.int32, (GROUP * q_len, proj), 1)
    ones = jnp.where(lane == 0, 1.0, 0.0).astype(jnp.bfloat16)

    @pl.loop(0, group_size // GROUP)
    def _(g):
        def arrived(count):
            view = all_q.at[pl.ds(0, count)]
            pltpu.make_async_copy(view, view, q_sem.at[g]).wait()

        @pl.when(g == 0)
        def _():
            arrived(GROUP - 1)

        @pl.when(g > 0)
        def _():
            arrived(GROUP)

        block = all_q[pl.ds(g * GROUP, GROUP)].reshape(GROUP * q_len, proj)
        block = jnp.concatenate([block, ones], axis=1)
        best = None
        for b in range(0, tokens.shape[0], SCORE_ROWS):
            sim = lax.dot_general(tokens[b:b + SCORE_ROWS, :], block, (((1,), (1,)), ((), ())),
                                  preferred_element_type=jnp.float32)
            part = jnp.max(sim.reshape(SCORE_ROWS // 8, 8, GROUP * q_len), axis=0)
            best = part if best is None else jnp.maximum(best, part)
        acc[g] = best

    top = jnp.max(acc[...], axis=1).reshape(group_size * q_len // 128, 128)
    per_row = 128 // q_len
    n_rows = group_size // per_row
    lane = lax.broadcasted_iota(jnp.int32, (n_rows, 128), 1)
    mine = jnp.zeros((1, 128), jnp.float32)
    for k in range(per_row):
        total = jnp.sum(jnp.where(lane // q_len == k, top, 0.0), axis=1, keepdims=True)
        mine += jnp.sum(jnp.where(lane == senders[k * n_rows:(k + 1) * n_rows, :], total, 0.0), axis=0, keepdims=True)
    column[...] = mine

    def s_copy(p):
        return pltpu.make_async_remote_copy(
            src_ref=column, dst_ref=table.at[row_of(p), :], send_sem=s_send_sem, recv_sem=s_sem,
            device_id=device_id(offsets[p]), device_id_type=MESH)

    for p in range(group_size - 1, 0, -1):
        s_copy(p).start()

    sent = all_q.at[pl.ds(0, group_size - 1)]
    pltpu.make_async_copy(sent, sent, send_sem).wait()
    others = table.at[pl.ds(0, group_size - 1), :]
    pltpu.make_async_copy(others, others, s_sem).wait()
    pltpu.make_async_copy(others, others, s_send_sem).wait()

    rows = lax.broadcasted_iota(jnp.int32, (group_size, 128), 0)
    out_ref[0] = jnp.where(rows == 0, mine, table[...])
    out_ref[1] = senders[...].astype(jnp.float32)


def finish(outer, inner, scores_ref, temp_ref, rows_ref, mean_ref):
    group_size = outer * inner
    me = lax.axis_index('data2') * inner + lax.axis_index('data')
    logits = scores_ref[0] / temp_ref[0]
    peak = jnp.max(logits, axis=0, keepdims=True)
    log_norm = peak + jnp.log(jnp.sum(jnp.exp(logits - peak), axis=0, keepdims=True))
    lane = lax.broadcasted_iota(jnp.int32, (group_size, 128), 1)
    own = lane == scores_ref[1].astype(jnp.int32)
    loss = log_norm - jnp.sum(jnp.where(own, logits, 0.0), axis=0, keepdims=True)
    lane = lane[:1]
    rows_ref[0] = jnp.sum(jnp.where(lane == me, loss, 0.0))
    mean_ref[0] = jnp.sum(jnp.where(lane < group_size, loss, 0.0)) / group_size


def solution(mesh):
    outer, inner = mesh.shape['data2'], mesh.shape['data']
    group_size = outer * inner

    def device_fn(q_hidden, d_hidden, w_proj, q_mask, d_mask, temperature):
        q_len, width = q_hidden.shape[1:]
        d_len, proj = d_hidden.shape[1], w_proj.shape[1]
        n_chunks = d_len // CHUNK
        smem = pl.BlockSpec(memory_space=pltpu.SMEM)
        vmem = pl.BlockSpec(memory_space=pltpu.VMEM)
        scores = pl.pallas_call(
            functools.partial(kernel, outer, inner),
            out_shape=jax.ShapeDtypeStruct((2, group_size, 128), jnp.float32),
            in_specs=[pl.BlockSpec(memory_space=pl.ANY)] * 5,
            out_specs=vmem,
            scratch_shapes=[
                pltpu.VMEM((n_chunks, CHUNK, width), jnp.bfloat16),
                pltpu.VMEM((2 * UNROLL, CHUNK, proj), jnp.float32),
                pltpu.VMEM((d_len, 2 * proj), jnp.bfloat16),
                pltpu.VMEM((group_size, q_len, proj), jnp.bfloat16),
                pltpu.VMEM((group_size // GROUP, 8, GROUP * q_len), jnp.float32),
                pltpu.VMEM((1, 128), jnp.float32),
                pltpu.VMEM((group_size, 128), jnp.float32),
                pltpu.VMEM((group_size, 128), jnp.int32),
                pltpu.VMEM(q_hidden.shape, q_hidden.dtype),
                pltpu.VMEM(w_proj.shape, w_proj.dtype),
                pltpu.VMEM(q_mask.shape, q_mask.dtype),
                pltpu.VMEM(d_mask.shape, d_mask.dtype),
                pltpu.SemaphoreType.DMA((4,)),
                pltpu.SemaphoreType.DMA((n_chunks,)),
                pltpu.SemaphoreType.DMA,
                pltpu.SemaphoreType.DMA((group_size // GROUP,)),
                pltpu.SemaphoreType.DMA,
                pltpu.SemaphoreType.DMA,
            ],
            compiler_params=pltpu.CompilerParams(collective_id=0, has_side_effects=True,
                                                 vmem_limit_bytes=60 * 1024 * 1024),
            name='colbert_loss',
        )(q_hidden, d_hidden, w_proj, q_mask, d_mask)
        return pl.pallas_call(
            functools.partial(finish, outer, inner),
            out_shape=(jax.ShapeDtypeStruct((1,), jnp.float32),) * 2,
            in_specs=[vmem, smem],
            out_specs=(smem, smem),
            name='loss',
        )(scores, temperature.reshape(1))

    return jax.shard_map(
        device_fn,
        mesh=mesh,
        in_specs=(P(ROW_AXES), P(ROW_AXES), P(), P(ROW_AXES), P(ROW_AXES), P()),
        out_specs=(P(ROW_AXES), P('replica')),
        check_vma=False,
    )
```

```python
import functools

import jax
import jax.numpy as jnp
from jax import lax
from jax.experimental import pallas as pl
from jax.experimental.pallas import tpu as pltpu
from jax.sharding import PartitionSpec as P

NORM_EPS = 1e-6
ROW_AXES = ('replica', 'data2', 'data')
MASKED = -1e30
CORES = 2
CHUNK = 512
DEPTH = 16
LEVELS = 2
RINGS = 1
FIRST = 2
STEPS = (1, 3, 4, 4, 4)
SEND_STEP = 2
SMALL_WAITS = ((0,), (1, 2, 3))
SCORE_ROWS = 4096
MESH = pl.DeviceIdType.MESH


def kernel(outer, inner, q_hbm, d_ref, w_hbm, qm_hbm, dm_hbm, out_ref,
           hidden, raw, tokens, all_q, acc, column, table, senders, q_ref, w_ref, qm_ref, dm_ref,
           small_sem, chunk_sem, send_sem, q_sem, s_send_sem, s_sem):
    part = all_q.shape[0] // (CORES * RINGS)
    group_size = outer * inner
    chips = inner // CORES
    q_len, proj = all_q.shape[1], w_ref.shape[1]
    n_chunks = hidden.shape[0]
    my_outer, my_inner = lax.axis_index('data2'), lax.axis_index('data')
    my_core = my_inner % CORES
    me = my_outer * inner + my_inner
    n_chips = group_size // CORES
    my_place = me // CORES
    my_ring = my_place // part
    my_slot = my_ring * CORES * part + my_place % part

    def chip_id(place):
        return {'data2': place // chips, 'data': place % chips * CORES + my_core}

    def other_chip(t):
        return t + 1 - (my_place + n_chips - 1 - t) // n_chips

    partner = {'data2': my_outer, 'data': my_inner + 1 - 2 * my_core}

    def row_of(p):
        per_row = 128 // q_len
        row = p % per_row * (group_size // per_row) + p // per_row
        return slice(row, row + 1)

    smalls = [pltpu.make_async_copy(src, dst, small_sem.at[i]) for i, (src, dst) in enumerate(
        [(w_hbm, w_ref), (q_hbm, q_ref), (qm_hbm, qm_ref), (dm_hbm, dm_ref)])]
    def fetch(b):
        return pltpu.make_async_copy(d_ref.at[0, pl.ds(b * CHUNK, CHUNK), :], hidden.at[b], chunk_sem.at[b])

    smalls[0].start()
    for b in range(FIRST):
        fetch(b).start(priority=min(b // FIRST, LEVELS - 1))
    barrier = pltpu.get_barrier_semaphore()
    for target in [chip_id(other_chip(t)) for t in range(n_chips - 1)] + [partner]:
        pl.semaphore_signal(barrier, inc=1, device_id=target, device_id_type=MESH)
    for copy in smalls[1:]:
        copy.start()
    for b in range(FIRST, DEPTH):
        fetch(b).start(priority=min(b // FIRST, LEVELS - 1))

    for p in range(group_size):
        place = p // (CORES * part) * part + p % part
        core = my_core if p // part % CORES == 0 else 1 - my_core
        senders[row_of(p), :] = jnp.full((1, 128), place * CORES + core, jnp.int32)
    def query():
        y = jnp.dot(q_ref[0], w_ref[...], preferred_element_type=jnp.float32)
        unit = y * lax.rsqrt(jnp.sum(y * y, axis=-1, keepdims=True) + NORM_EPS)
        row = lax.broadcasted_iota(jnp.int32, (q_len, q_len), 0)
        col = lax.broadcasted_iota(jnp.int32, (q_len, q_len), 1)
        weight = jnp.sum(jnp.where(row == col, qm_ref[...], 0).astype(jnp.float32), axis=1, keepdims=True)
        all_q[my_slot] = jnp.where(weight > 0, unit, 0.0).astype(jnp.bfloat16)

    def q_copy(t):
        return pltpu.make_async_remote_copy(
            src_ref=all_q.at[my_slot], dst_ref=all_q.at[my_slot], send_sem=send_sem.at[0], recv_sem=q_sem.at[my_ring * CORES],
            device_id=chip_id(other_chip(t)), device_id_type=MESH)

    def forward(r):
        return pltpu.make_async_remote_copy(
            src_ref=all_q.at[pl.ds(CORES * r * part, part)], dst_ref=all_q.at[pl.ds((CORES * r + 1) * part, part)],
            send_sem=send_sem.at[1 + r], recv_sem=q_sem.at[CORES * r + 1], device_id=partner, device_id_type=MESH)

    def project(b):
        raw[b] = jnp.dot(hidden[b], w_ref[...], preferred_element_type=jnp.float32)

    def normalise(b):
        y = raw[b]
        scale = lax.rsqrt(jnp.sum(y * y, axis=-1, keepdims=True) + NORM_EPS)
        rows = slice(b * CHUNK, (b + 1) * CHUNK)
        tokens[rows, :proj] = (y * scale).astype(jnp.bfloat16)
        bias = jnp.where(dm_ref[:, rows] > 0, 0.0, MASKED)
        for c in range(0, CHUNK, 128):
            block = jnp.broadcast_to(bias[:, c:c + 128], (128, 128)).T
            tokens[b * CHUNK + c:b * CHUNK + c + 128, proj:] = block.astype(jnp.bfloat16)

    chunks, ready = list(range(n_chunks)), []
    for i, count in enumerate(STEPS):
        now, chunks = chunks[:count], chunks[count:]
        if i == SEND_STEP:
            pl.semaphore_wait(barrier, n_chips)
            for t in reversed(range(n_chips - 1)):
                q_copy(t).start()
        for b in now:
            fetch(b).wait()
            if b + DEPTH < n_chunks:
                fetch(b + DEPTH).start()
        if i < len(SMALL_WAITS):
            for k in SMALL_WAITS[i]:
                smalls[k].wait()
        for b in ready:
            normalise(b)
        if i == 1:
            query()
        for b in now:
            project(b)
        ready = now

    lane = lax.broadcasted_iota(jnp.int32, (part * q_len, proj), 1)
    ones = jnp.where(lane == 0, 1.0, 0.0).astype(jnp.bfloat16)
    for g in range(CORES * RINGS):
        r = g // CORES
        if g % CORES == 0:
            rest, last = all_q.at[pl.ds(0, part - 1)], all_q.at[0]
            pltpu.make_async_copy(rest, rest, q_sem.at[g]).wait()

            @pl.when(my_ring != r)
            def _():
                pltpu.make_async_copy(last, last, q_sem.at[g]).wait()

            forward(r).start()
        else:
            forward(r).wait()
        for b in ready:
            normalise(b)
        ready = []
        block = all_q[g * part:(g + 1) * part].reshape(part * q_len, proj)
        block = jnp.concatenate([block, ones], axis=1)
        best = None
        for b in range(0, tokens.shape[0], SCORE_ROWS):
            sim = lax.dot_general(tokens[b:b + SCORE_ROWS, :], block, (((1,), (1,)), ((), ())),
                                  preferred_element_type=jnp.float32)
            best_b = jnp.max(sim.reshape(SCORE_ROWS // 8, 8, part * q_len), axis=0)
            best = best_b if best is None else jnp.maximum(best, best_b)
        acc[g] = best

    top = jnp.max(acc[...], axis=1).reshape(group_size * q_len // 128, 128)
    per_row = 128 // q_len
    n_rows = group_size // per_row
    lane = lax.broadcasted_iota(jnp.int32, (n_rows, 128), 1)
    mine = jnp.zeros((1, 128), jnp.float32)
    for k in range(per_row):
        total = jnp.sum(jnp.where(lane // q_len == k, top, 0.0), axis=1, keepdims=True)
        mine += jnp.sum(jnp.where(lane == senders[k * n_rows:(k + 1) * n_rows, :], total, 0.0), axis=0, keepdims=True)
    column[...] = mine

    def s_copy(t):
        target = t + 1 - (me + group_size - 1 - t) // group_size
        return pltpu.make_async_remote_copy(
            src_ref=column, dst_ref=table.at[pl.ds(me, 1), :], send_sem=s_send_sem, recv_sem=s_sem,
            device_id={'data2': target // inner, 'data': target % inner}, device_id_type=MESH)

    for t in range(group_size - 1):
        s_copy(t).start()

    sent = all_q.at[pl.ds(0, n_chips - 1)]
    pltpu.make_async_copy(sent, sent, send_sem.at[0]).wait()
    others = table.at[pl.ds(0, group_size - 1), :]
    pltpu.make_async_copy(others, others, s_sem).wait()
    pltpu.make_async_copy(others, others, s_send_sem).wait()

    rows = lax.broadcasted_iota(jnp.int32, (group_size, 128), 0)
    out_ref[...] = jnp.where(rows == me, mine, table[...])


def finish(outer, inner, scores_ref, temp_ref, rows_ref, mean_ref):
    group_size = outer * inner
    me = lax.axis_index('data2') * inner + lax.axis_index('data')
    logits = scores_ref[...] / temp_ref[0]
    peak = jnp.max(logits, axis=0, keepdims=True)
    log_norm = peak + jnp.log(jnp.sum(jnp.exp(logits - peak), axis=0, keepdims=True))
    lane = lax.broadcasted_iota(jnp.int32, (group_size, 128), 1)
    own = lane == lax.broadcasted_iota(jnp.int32, (group_size, 128), 0)
    loss = log_norm - jnp.sum(jnp.where(own, logits, 0.0), axis=0, keepdims=True)
    lane = lane[:1]
    rows_ref[0] = jnp.sum(jnp.where(lane == me, loss, 0.0))
    mean_ref[0] = jnp.sum(jnp.where(lane < group_size, loss, 0.0)) / group_size


def solution(mesh):
    outer, inner = mesh.shape['data2'], mesh.shape['data']
    group_size = outer * inner

    def device_fn(q_hidden, d_hidden, w_proj, q_mask, d_mask, temperature):
        q_len, width = q_hidden.shape[1:]
        d_len, proj = d_hidden.shape[1], w_proj.shape[1]
        n_chunks = d_len // CHUNK
        smem = pl.BlockSpec(memory_space=pltpu.SMEM)
        vmem = pl.BlockSpec(memory_space=pltpu.VMEM)
        scores = pl.pallas_call(
            functools.partial(kernel, outer, inner),
            out_shape=pltpu.VMEM((group_size, 128), jnp.float32),
            in_specs=[pl.BlockSpec(memory_space=pl.ANY)] * 5,
            out_specs=vmem,
            scratch_shapes=[
                pltpu.VMEM((n_chunks, CHUNK, width), jnp.bfloat16),
                pltpu.VMEM((n_chunks, CHUNK, proj), jnp.float32),
                pltpu.VMEM((d_len, 2 * proj), jnp.bfloat16),
                pltpu.VMEM((group_size, q_len, proj), jnp.bfloat16),
                pltpu.VMEM((CORES * RINGS, 8, group_size // (CORES * RINGS) * q_len), jnp.float32),
                pltpu.VMEM((1, 128), jnp.float32),
                pltpu.VMEM((group_size, 128), jnp.float32),
                pltpu.VMEM((group_size, 128), jnp.int32),
                pltpu.VMEM(q_hidden.shape, q_hidden.dtype),
                pltpu.VMEM(w_proj.shape, w_proj.dtype),
                pltpu.VMEM(q_mask.shape, q_mask.dtype),
                pltpu.VMEM(d_mask.shape, d_mask.dtype),
                pltpu.SemaphoreType.DMA((4,)),
                pltpu.SemaphoreType.DMA((n_chunks,)),
                pltpu.SemaphoreType.DMA((1 + RINGS,)),
                pltpu.SemaphoreType.DMA((CORES * RINGS,)),
                pltpu.SemaphoreType.DMA,
                pltpu.SemaphoreType.DMA,
            ],
            compiler_params=pltpu.CompilerParams(collective_id=0, has_side_effects=True,
                                                 vmem_limit_bytes=60 * 1024 * 1024),
            name='colbert_loss',
        )(q_hidden, d_hidden, w_proj, q_mask, d_mask)
        return pl.pallas_call(
            functools.partial(finish, outer, inner),
            out_shape=(jax.ShapeDtypeStruct((1,), jnp.float32),) * 2,
            in_specs=[vmem, smem],
            out_specs=(smem, smem),
            compiler_params=pltpu.CompilerParams(vmem_limit_bytes=4 * 1024 * 1024),
            name='loss',
        )(scores, temperature.reshape(1))

    return jax.shard_map(
        device_fn,
        mesh=mesh,
        in_specs=(P(ROW_AXES), P(ROW_AXES), P(), P(ROW_AXES), P(ROW_AXES), P()),
        out_specs=(P(ROW_AXES), P('replica')),
        check_vma=False,
    )
```

```python
import functools

import jax
import jax.numpy as jnp
from jax import lax
from jax.experimental import pallas as pl
from jax.experimental.pallas import tpu as pltpu
from jax.sharding import PartitionSpec as P

NORM_EPS = 1e-6
ROW_AXES = ('replica', 'data2', 'data')
MASKED = -1e30
CORES = 2
CHUNK = 512
DEPTH = 16
LEVELS = 2
RINGS = 1
FIRST = 2
STEPS = (1, 2, 4, 4, 5)
SEND_STEP = 2
SMALL_WAITS = ((0,), (1, 2, 3))
SCORE_ROWS = 4096
MESH = pl.DeviceIdType.MESH


def kernel(outer, inner, q_hbm, d_ref, w_hbm, qm_hbm, dm_hbm, out_ref,
           hidden, raw, tokens, all_q, acc, column, table, senders, q_ref, w_ref, qm_ref, dm_ref,
           small_sem, chunk_sem, send_sem, q_sem, s_send_sem, s_sem):
    part = all_q.shape[0] // (CORES * RINGS)
    group_size = outer * inner
    chips = inner // CORES
    q_len, proj = all_q.shape[1], w_ref.shape[1]
    n_chunks = hidden.shape[0]
    my_outer, my_inner = lax.axis_index('data2'), lax.axis_index('data')
    my_core = my_inner % CORES
    me = my_outer * inner + my_inner
    n_chips = group_size // CORES
    my_place = me // CORES
    my_ring = my_place // part
    my_slot = my_ring * CORES * part + my_place % part

    def chip_id(place):
        return {'data2': place // chips, 'data': place % chips * CORES + my_core}

    def other_chip(t):
        return t + 1 - (my_place + n_chips - 1 - t) // n_chips

    partner = {'data2': my_outer, 'data': my_inner + 1 - 2 * my_core}

    def row_of(p):
        per_row = 128 // q_len
        row = p % per_row * (group_size // per_row) + p // per_row
        return slice(row, row + 1)

    smalls = [pltpu.make_async_copy(src, dst, small_sem.at[i]) for i, (src, dst) in enumerate(
        [(w_hbm, w_ref), (q_hbm, q_ref), (qm_hbm, qm_ref), (dm_hbm, dm_ref)])]
    def fetch(b):
        return pltpu.make_async_copy(d_ref.at[0, pl.ds(b * CHUNK, CHUNK), :], hidden.at[b], chunk_sem.at[b])

    smalls[0].start()
    for b in range(FIRST):
        fetch(b).start(priority=min(b // FIRST, LEVELS - 1))
    barrier = pltpu.get_barrier_semaphore()
    for target in [chip_id(other_chip(t)) for t in range(n_chips - 1)] + [partner]:
        pl.semaphore_signal(barrier, inc=1, device_id=target, device_id_type=MESH)
    for copy in smalls[1:]:
        copy.start()
    for b in range(FIRST, DEPTH):
        fetch(b).start(priority=min(b // FIRST, LEVELS - 1))

    for p in range(group_size):
        place = p // (CORES * part) * part + p % part
        core = my_core if p // part % CORES == 0 else 1 - my_core
        senders[row_of(p), :] = jnp.full((1, 128), place * CORES + core, jnp.int32)
    def query():
        y = jnp.dot(q_ref[0], w_ref[...], preferred_element_type=jnp.float32)
        unit = y * lax.rsqrt(jnp.sum(y * y, axis=-1, keepdims=True) + NORM_EPS)
        row = lax.broadcasted_iota(jnp.int32, (q_len, q_len), 0)
        col = lax.broadcasted_iota(jnp.int32, (q_len, q_len), 1)
        weight = jnp.sum(jnp.where(row == col, qm_ref[...], 0).astype(jnp.float32), axis=1, keepdims=True)
        all_q[my_slot] = jnp.where(weight > 0, unit, 0.0).astype(jnp.bfloat16)

    def q_copy(t):
        return pltpu.make_async_remote_copy(
            src_ref=all_q.at[my_slot], dst_ref=all_q.at[my_slot], send_sem=send_sem.at[0], recv_sem=q_sem.at[my_ring * CORES],
            device_id=chip_id((my_place + n_chips // 2 + t + (t >= n_chips // 2)) % n_chips), device_id_type=MESH)

    def forward(r):
        return pltpu.make_async_remote_copy(
            src_ref=all_q.at[pl.ds(CORES * r * part, part)], dst_ref=all_q.at[pl.ds((CORES * r + 1) * part, part)],
            send_sem=send_sem.at[1 + r], recv_sem=q_sem.at[CORES * r + 1], device_id=partner, device_id_type=MESH)

    def project(b):
        raw[b] = jnp.dot(hidden[b], w_ref[...], preferred_element_type=jnp.float32)

    def normalise(b):
        y = raw[b]
        scale = lax.rsqrt(jnp.sum(y * y, axis=-1, keepdims=True) + NORM_EPS)
        rows = slice(b * CHUNK, (b + 1) * CHUNK)
        tokens[rows, :proj] = (y * scale).astype(jnp.bfloat16)
        bias = jnp.where(dm_ref[:, rows] > 0, 0.0, MASKED)
        for c in range(0, CHUNK, 128):
            block = jnp.broadcast_to(bias[:, c:c + 128], (128, 128)).T
            tokens[b * CHUNK + c:b * CHUNK + c + 128, proj:] = block.astype(jnp.bfloat16)

    chunks, ready = list(range(n_chunks)), []
    for i, count in enumerate(STEPS):
        now, chunks = chunks[:count], chunks[count:]
        if i == SEND_STEP:
            pl.semaphore_wait(barrier, n_chips)
            for t in range(n_chips - 1):
                q_copy(t).start()
        for b in now:
            fetch(b).wait()
            if b + DEPTH < n_chunks:
                fetch(b + DEPTH).start()
        if i < len(SMALL_WAITS):
            for k in SMALL_WAITS[i]:
                smalls[k].wait()
        for b in ready:
            normalise(b)
        if i == 1:
            query()
        for b in now:
            project(b)
        ready = now

    lane = lax.broadcasted_iota(jnp.int32, (part * q_len, proj), 1)
    ones = jnp.where(lane == 0, 1.0, 0.0).astype(jnp.bfloat16)
    for g in range(CORES * RINGS):
        r = g // CORES
        if g % CORES == 0:
            rest, last = all_q.at[pl.ds(0, part - 1)], all_q.at[0]
            pltpu.make_async_copy(rest, rest, q_sem.at[g]).wait()

            @pl.when(my_ring != r)
            def _():
                pltpu.make_async_copy(last, last, q_sem.at[g]).wait()

            forward(r).start()
        else:
            forward(r).wait()
        for b in ready:
            normalise(b)
        ready = []
        block = all_q[g * part:(g + 1) * part].reshape(part * q_len, proj)
        block = jnp.concatenate([block, ones], axis=1)
        best = None
        for b in range(0, tokens.shape[0], SCORE_ROWS):
            sim = lax.dot_general(tokens[b:b + SCORE_ROWS, :], block, (((1,), (1,)), ((), ())),
                                  preferred_element_type=jnp.float32)
            best_b = jnp.max(sim.reshape(SCORE_ROWS // 8, 8, part * q_len), axis=0)
            best = best_b if best is None else jnp.maximum(best, best_b)
        acc[g] = best

    top = jnp.max(acc[...], axis=1).reshape(group_size * q_len // 128, 128)
    per_row = 128 // q_len
    n_rows = group_size // per_row
    lane = lax.broadcasted_iota(jnp.int32, (n_rows, 128), 1)
    mine = jnp.zeros((1, 128), jnp.float32)
    for k in range(per_row):
        total = jnp.sum(jnp.where(lane // q_len == k, top, 0.0), axis=1, keepdims=True)
        mine += jnp.sum(jnp.where(lane == senders[k * n_rows:(k + 1) * n_rows, :], total, 0.0), axis=0, keepdims=True)
    column[...] = mine

    def s_copy(t):
        target = t + 1 - (me + group_size - 1 - t) // group_size
        return pltpu.make_async_remote_copy(
            src_ref=column, dst_ref=table.at[pl.ds(me, 1), :], send_sem=s_send_sem, recv_sem=s_sem,
            device_id={'data2': target // inner, 'data': target % inner}, device_id_type=MESH)

    for t in range(group_size - 1):
        s_copy(t).start()

    sent = all_q.at[pl.ds(0, n_chips - 1)]
    pltpu.make_async_copy(sent, sent, send_sem.at[0]).wait()
    others = table.at[pl.ds(0, group_size - 1), :]
    pltpu.make_async_copy(others, others, s_sem).wait()
    pltpu.make_async_copy(others, others, s_send_sem).wait()

    rows = lax.broadcasted_iota(jnp.int32, (group_size, 128), 0)
    out_ref[...] = jnp.where(rows == me, mine, table[...])


def finish(outer, inner, scores_ref, temp_ref, rows_ref, mean_ref):
    group_size = outer * inner
    me = lax.axis_index('data2') * inner + lax.axis_index('data')
    logits = scores_ref[...] / temp_ref[0]
    peak = jnp.max(logits, axis=0, keepdims=True)
    log_norm = peak + jnp.log(jnp.sum(jnp.exp(logits - peak), axis=0, keepdims=True))
    lane = lax.broadcasted_iota(jnp.int32, (group_size, 128), 1)
    own = lane == lax.broadcasted_iota(jnp.int32, (group_size, 128), 0)
    loss = log_norm - jnp.sum(jnp.where(own, logits, 0.0), axis=0, keepdims=True)
    lane = lane[:1]
    rows_ref[...] = jnp.sum(jnp.where(lane == me, loss, 0.0), axis=1)
    mean_ref[...] = jnp.sum(jnp.where(lane < group_size, loss, 0.0), axis=1) / group_size


def solution(mesh):
    outer, inner = mesh.shape['data2'], mesh.shape['data']
    group_size = outer * inner

    def device_fn(q_hidden, d_hidden, w_proj, q_mask, d_mask, temperature):
        q_len, width = q_hidden.shape[1:]
        d_len, proj = d_hidden.shape[1], w_proj.shape[1]
        n_chunks = d_len // CHUNK
        smem = pl.BlockSpec(memory_space=pltpu.SMEM)
        vmem = pl.BlockSpec(memory_space=pltpu.VMEM)
        scores = pl.pallas_call(
            functools.partial(kernel, outer, inner),
            out_shape=pltpu.VMEM((group_size, 128), jnp.float32),
            in_specs=[pl.BlockSpec(memory_space=pl.ANY)] * 5,
            out_specs=vmem,
            scratch_shapes=[
                pltpu.VMEM((n_chunks, CHUNK, width), jnp.bfloat16),
                pltpu.VMEM((n_chunks, CHUNK, proj), jnp.float32),
                pltpu.VMEM((d_len, 2 * proj), jnp.bfloat16),
                pltpu.VMEM((group_size, q_len, proj), jnp.bfloat16),
                pltpu.VMEM((CORES * RINGS, 8, group_size // (CORES * RINGS) * q_len), jnp.float32),
                pltpu.VMEM((1, 128), jnp.float32),
                pltpu.VMEM((group_size, 128), jnp.float32),
                pltpu.VMEM((group_size, 128), jnp.int32),
                pltpu.VMEM(q_hidden.shape, q_hidden.dtype),
                pltpu.VMEM(w_proj.shape, w_proj.dtype),
                pltpu.VMEM(q_mask.shape, q_mask.dtype),
                pltpu.VMEM(d_mask.shape, d_mask.dtype),
                pltpu.SemaphoreType.DMA((4,)),
                pltpu.SemaphoreType.DMA((n_chunks,)),
                pltpu.SemaphoreType.DMA((1 + RINGS,)),
                pltpu.SemaphoreType.DMA((CORES * RINGS,)),
                pltpu.SemaphoreType.DMA,
                pltpu.SemaphoreType.DMA,
            ],
            compiler_params=pltpu.CompilerParams(collective_id=0, has_side_effects=True,
                                                 vmem_limit_bytes=60 * 1024 * 1024),
            name='colbert_loss',
        )(q_hidden, d_hidden, w_proj, q_mask, d_mask)
        return pl.pallas_call(
            functools.partial(finish, outer, inner),
            out_shape=(jax.ShapeDtypeStruct((1,), jnp.float32),) * 2,
            in_specs=[vmem, smem],
            out_specs=(vmem, vmem),
            compiler_params=pltpu.CompilerParams(vmem_limit_bytes=4 * 1024 * 1024),
            name='loss',
        )(scores, temperature.reshape(1))

    return jax.shard_map(
        device_fn,
        mesh=mesh,
        in_specs=(P(ROW_AXES), P(ROW_AXES), P(), P(ROW_AXES), P(ROW_AXES), P()),
        out_specs=(P(ROW_AXES), P('replica')),
        check_vma=False,
    )
```
